32 devices in a mesh: section: 4 (over y, core), tp: 8 (over z, x).
Axes of the slice: x: 2, y: 2, z: 4, core: 2. Of those that a mesh axis runs over, the one named last changes fastest.
Arguments:
- token_ids: int32 [2, 128], replicated, may hold values from 0 to 65535
- alpha_num: int32 [1], replicated, may hold values from 3 to 7
- embed_table: bfloat16 [65536, 8192], P('section', 'tp'), may hold values from -6 to 6
- norm_gain: float32 [4, 8192], P('section'), may hold values from 0.5 to 1.5
- w_query: bfloat16 [4, 8192, 4096], P('section', None, 'tp'), may hold values from -4 to 4
- w_key: bfloat16 [4, 8192, 512], P('section', None, 'tp'), may hold values from -4 to 4
- w_value: bfloat16 [4, 8192, 512], P('section', None, 'tp'), may hold values from -0.0625 to 0.0625
- w_out: bfloat16 [4, 4096, 8192], P('section', 'tp'), may hold values from -0.09375 to 0.09375
Outputs:
- layer_out: bfloat16 [4, 2, 128, 8192], P('section', None, 'tp')
- scales_in: float32 [4, 8192], P('section')
- scales_out: float32 [4, 4096], P('section', 'tp')
- smoothed_q: bfloat16 [4, 8192, 4096], P('section', None, 'tp')
- smoothed_k: bfloat16 [4, 8192, 512], P('section', None, 'tp')
- smoothed_v: bfloat16 [4, 8192, 512], P('section', None, 'tp')
The draws below stay inside these ranges and needn't reach their ends.
All inputs are finite; a program needn't handle non-finite values.
Results may differ from the reference program's by a relative error of at most 0.028.
Values may be sent and summed in bfloat16 or wider, within the bound.
A program may use at most 128 MiB of HBM per device.

```python
import math
import jax
import jax.numpy as jnp
import numpy as np
from jax import lax

D = 8192
HEADS = 32
KV_HEADS = 4
HEAD_DIM = 128
VOCAB = 65536
SEQ = 128
MICRO = 2
LAYERS = 4
QD = 4096
KVD = 512
N_TP = 8


def draw_w_key(key, part):
    fresh = jax.random.normal(jax.random.fold_in(key, 23), (LAYERS, D, KV_HEADS * HEAD_DIM), jnp.float32)
    return (fresh / math.sqrt(D)).astype(jnp.bfloat16)


def draw_w_query(key, part):
    noise = jax.random.normal(jax.random.fold_in(key, 29), (LAYERS, D, HEADS * HEAD_DIM), jnp.float32) / math.sqrt(D)
    return noise.astype(jnp.bfloat16)


def plant(drawn, rng, least, largest):
    place = [jax.random.randint(jax.random.fold_in(rng, axis), (), 0, length) for axis, length in enumerate(drawn.shape)]
    main_axis = drawn.shape.index(max(drawn.shape))
    next_to = place[:main_axis] + [(place[main_axis] + 1) % drawn.shape[main_axis]] + place[main_axis + 1:]
    return drawn.at[tuple(place)].set(least).at[tuple(next_to)].set(largest)


def shard_levels(rng, shape, split, smallest, largest):
    def one(dim, blocks):
        heights = jax.random.uniform(jax.random.fold_in(jax.random.fold_in(rng, 6), dim), (blocks,), jnp.float32, smallest / len(split), largest / len(split))
        return jnp.repeat(jnp.exp(heights), shape[dim] // blocks).reshape((-1,) + (1,) * (len(shape) - dim - 1))

    gain = one(*split[0])
    for cut in split[1:]:
        gain = gain * one(*cut)
    return gain


def rank_table(amount, slope):
    portions = [(1 << 20) // math.isqrt(standing ** slope) + 1 for standing in range(1, amount + 1)]
    width = 1 + sum(portions) // (1 << 30)
    return np.cumsum(np.array([max(1, weight // width) for weight in portions]))


def ranked(rng, extent, count, skew):
    listing = rank_table(count, skew)
    lot = jax.random.randint(jax.random.fold_in(rng, 1), extent, 0, int(listing[count - 1]))
    rank = jnp.searchsorted(jnp.asarray(listing, jnp.int32), lot, side="right")
    return jax.random.permutation(jax.random.fold_in(rng, 2), count)[rank].astype(jnp.int32)


def centred(rng, shape, width, limit, split=(), held_as=jnp.bfloat16):
    result = jax.random.normal(rng, shape, jnp.float32) * width
    if len(split) > 0:
        result = shard_levels(rng, shape, split, -0.22, 0.18) * result
    return jnp.clip(result, min=-limit, max=limit).astype(held_as)


def setup_inputs(seed: int = 0) -> dict:
    keys = jax.random.split(jax.random.key(seed), 9)
    return {
        "token_ids": plant(ranked(keys[0], (MICRO, SEQ), VOCAB, 2), jax.random.fold_in(keys[0], 3), 0, VOCAB - 1).astype(jnp.int32),
        "alpha_num": jax.random.randint(keys[1], (1,), 3, 8).astype(jnp.int32),
        "embed_table": centred(keys[2], (VOCAB, D), 1.0, 6.0, ((0, 4), (1, 8))),
        "norm_gain": jnp.clip(1.0 + 0.1 * jax.random.normal(keys[3], (LAYERS, D), jnp.float32), 0.5, 1.5),
        "w_query": draw_w_query(jax.random.fold_in(keys[8], 71), 0),
        "w_key": draw_w_key(jax.random.fold_in(keys[8], 71), 0),
        "w_value": centred(keys[6], (LAYERS, D, KVD), D ** -0.5, 0.0625, ((0, 4), (2, 8))),
        "w_out": centred(keys[7], (LAYERS, QD, D), QD ** -0.5, 0.09375, ((0, 4), (1, 8))),
    }


norm_eps = 1e-05
stat_eps = 1e-05
rope_base = 500000.0

def rope_tables(length, head_size):
    halves = head_size // 2
    freqs = jnp.exp(-math.log(rope_base) * 2.0 * jnp.arange(halves, dtype=jnp.float32) / head_size)
    angles = jnp.arange(length, dtype=jnp.float32)[:, None] * freqs[None, :]
    return (jnp.cos(angles), jnp.sin(angles))

def rotate(values, cosine, sine):
    halves = values.shape[-1] // 2
    lower = values[..., :halves]
    upper = values[..., halves:]
    cos_rows = cosine[:, None, :]
    sin_rows = sine[:, None, :]
    return jnp.concatenate([lower * cos_rows - upper * sin_rows, upper * cos_rows + lower * sin_rows], axis=-1)

def smoothing(act_peak, weight_peak, alpha_exp):
    return jnp.exp(alpha_exp * jnp.log(act_peak + stat_eps) - (1.0 - alpha_exp) * jnp.log(weight_peak + stat_eps))

def attention_layer(resid, gain_row, query_w, key_w, value_w, out_w):
    length = resid.shape[0]
    values = resid.astype(jnp.float32)
    square = lax.optimization_barrier(jnp.mean(values * values, axis=1, keepdims=True))
    normed = (values * lax.rsqrt(square + norm_eps) * gain_row[None, :]).astype(jnp.bfloat16)
    query = jnp.dot(normed, query_w, preferred_element_type=jnp.float32)
    key_rows = lax.optimization_barrier(jnp.dot(normed, key_w, preferred_element_type=jnp.float32).astype(jnp.bfloat16))
    value_rows = jnp.dot(normed, value_w, preferred_element_type=jnp.float32).astype(jnp.bfloat16)
    cosine, sine = rope_tables(length, HEAD_DIM)
    query_rot = rotate(query.reshape(length, HEADS, HEAD_DIM), cosine, sine).astype(jnp.bfloat16)
    key_rot = rotate(key_rows.astype(jnp.float32).reshape(length, KV_HEADS, HEAD_DIM), cosine, sine).astype(jnp.bfloat16)
    group_size = HEADS // KV_HEADS
    grouped = query_rot.reshape(length, group_size, KV_HEADS, HEAD_DIM).astype(jnp.float32)
    scores = jnp.einsum('qrgd,kgd->grqk', grouped, key_rot.astype(jnp.float32)) / math.sqrt(HEAD_DIM)
    positions = jnp.arange(length, dtype=jnp.int32)
    causal = positions[:, None] >= positions[None, :]
    scores = jnp.where(causal[None, None], scores, -1e+30)
    probs = jax.nn.softmax(scores, axis=-1).astype(jnp.bfloat16)
    value_heads = value_rows.reshape(length, KV_HEADS, HEAD_DIM).astype(jnp.float32)
    attended = jnp.einsum('grqk,kgd->qrgd', probs.astype(jnp.float32), value_heads)
    attended = attended.reshape(length, HEADS * HEAD_DIM).astype(jnp.bfloat16)
    group_cols = HEADS * HEAD_DIM // N_TP
    head_parts = jnp.einsum('qnc,ncd->nqd', attended.reshape(length, N_TP, group_cols).astype(jnp.float32), out_w.reshape(N_TP, group_cols, D).astype(jnp.float32)).astype(jnp.bfloat16)
    mixed = lax.optimization_barrier(jnp.sum(head_parts.astype(jnp.float32), axis=0))
    output = lax.optimization_barrier((values + mixed).astype(jnp.bfloat16))
    normed_peak = lax.optimization_barrier(jnp.max(jnp.abs(normed), axis=0)).astype(jnp.float32)
    attended_peak = lax.optimization_barrier(jnp.max(jnp.abs(attended), axis=0)).astype(jnp.float32)
    return (output, normed_peak, attended_peak)

def reference(token_ids, alpha_num, embed_table, norm_gain, w_query, w_key, w_value, w_out):
    alpha_exp = alpha_num[0].astype(jnp.float32) / 10.0
    stream = jnp.take(embed_table, token_ids, axis=0)
    outputs = []
    inputs_scales = []
    output_scales = []
    smooth_query = []
    smooth_key = []
    smooth_value = []
    for layer_index in range(LAYERS):

        def advance(carry, resid):
            act_peak, head_peak = carry
            output, normed_peak, attended_peak = attention_layer(resid, norm_gain[layer_index], w_query[layer_index], w_key[layer_index], w_value[layer_index], w_out[layer_index])
            return ((jnp.maximum(act_peak, normed_peak), jnp.maximum(head_peak, attended_peak)), output)
        start_peaks = (jnp.zeros((D,), jnp.float32), jnp.zeros((HEADS * HEAD_DIM,), jnp.float32))
        (act_peak, head_peak), stream = lax.scan(advance, start_peaks, stream)
        outputs.append(stream)
        weight_peak = jnp.maximum(jnp.maximum(lax.optimization_barrier(jnp.max(jnp.abs(w_query[layer_index]), axis=1)), lax.optimization_barrier(jnp.max(jnp.abs(w_key[layer_index]), axis=1))), lax.optimization_barrier(jnp.max(jnp.abs(w_value[layer_index]), axis=1))).astype(jnp.float32)
        out_peak = lax.optimization_barrier(jnp.max(jnp.abs(w_out[layer_index]), axis=1)).astype(jnp.float32)
        scale_in = smoothing(act_peak, weight_peak, alpha_exp)
        scale_out = smoothing(head_peak, out_peak, alpha_exp)
        inputs_scales.append(scale_in)
        output_scales.append(scale_out)
        smooth_query.append((w_query[layer_index].astype(jnp.float32) * scale_in[:, None]).astype(jnp.bfloat16))
        smooth_key.append((w_key[layer_index].astype(jnp.float32) * scale_in[:, None]).astype(jnp.bfloat16))
        smooth_value.append((w_value[layer_index].astype(jnp.float32) * scale_in[:, None]).astype(jnp.bfloat16))
    return (jnp.stack(outputs), jnp.stack(inputs_scales), jnp.stack(output_scales), jnp.stack(smooth_query), jnp.stack(smooth_key), jnp.stack(smooth_value))
```

```python
import contextlib
import functools
import math

import jax
import jax.numpy as jnp
from jax import lax
from jax.experimental import pallas as pl
from jax.experimental.pallas import tpu as pltpu
from jax.sharding import PartitionSpec as P

KV_HEADS = 4
HEAD_DIM = 128


norm_eps = 1e-05
stat_eps = 1e-05
rope_base = 500000.0


def rope_tables(length, head_size):
    halves = head_size // 2
    freqs = jnp.exp(-math.log(rope_base) * 2.0 * jnp.arange(halves, dtype=jnp.float32) / head_size)
    angles = jnp.arange(length, dtype=jnp.float32)[:, None] * freqs[None, :]
    return (jnp.cos(angles), jnp.sin(angles))


def smoothing(act_peak, weight_peak, alpha_exp):
    return jnp.exp(
        alpha_exp * jnp.log(act_peak + stat_eps)
        - (1.0 - alpha_exp) * jnp.log(weight_peak + stat_eps)
    )


MESH = pl.DeviceIdType.MESH
TILE = 512
LANES = 128


def scope(name):
    return contextlib.nullcontext()


def remote(src, dst, send, recv, where):
    return pltpu.make_async_remote_copy(
        src_ref=src, dst_ref=dst, send_sem=send, recv_sem=recv, device_id=where, device_id_type=MESH
    )


def grid_of(count):
    minor = 1
    while (2 * minor) * (2 * minor) <= count and count % (2 * minor) == 0:
        minor *= 2
    return (count // minor, minor)


def levels_of(sections):
    distances = []
    while (1 << len(distances)) < sections:
        distances.append(1 << len(distances))
    return distances


def layers_kernel(
    sections,
    count,
    picked,
    gain,
    wq,
    wk,
    wv,
    wo,
    cos2,
    sin2,
    out,
    act_out,
    head_out,
    wpeak_out,
    opeak_out,
    emb,
    emb_acc,
    xall,
    ssq,
    acc_q,
    acc_kv,
    kvbuf,
    krot,
    vall,
    att,
    part,
    r1,
    s2,
    r2,
    own,
    wpeak,
    wpbuf,
    emb_s,
    emb_r,
    col_s,
    fwd_s,
    on_s,
    ag_r,
    kv_s,
    kv_r,
    r1_s,
    r1_r,
    s2_s,
    r2_r,
    wp_s,
    wp_r,
):
    major, minor = grid_of(count)
    section = lax.axis_index("section")
    me = lax.axis_index("tp")
    a = me // minor
    b = me % minor
    micros, _, rows, feats = picked.shape
    width = feats * count
    length = rows * count
    query_cols = wq.shape[1]
    kv_cols = wk.shape[0]
    heads_here = query_cols // HEAD_DIM
    per_head = HEAD_DIM // kv_cols
    chunks = major
    span = width // chunks
    distances = levels_of(sections)
    later = (section + sections - 1) // sections

    def peer(number):
        return (section, number)

    def col_peer(step):
        return lax.rem(a + step + major, major)

    def row_peer(step):
        return lax.rem(b + step + minor, minor)

    with scope("p_barrier"):
        barrier = pltpu.get_barrier_semaphore()
        for step in range(1, count):
            pl.semaphore_signal(
                barrier, inc=1, device_id=peer(lax.rem(me + step, count)), device_id_type=MESH
            )

        @pl.when(section > 0)
        def _():
            for step in range(major):
                pl.semaphore_signal(
                    barrier,
                    inc=1,
                    device_id=(section - 1, col_peer(step) * minor + b),
                    device_id_type=MESH,
                )

        @pl.when(section < sections - 1)
        def _():
            for step in range(major):
                pl.semaphore_signal(
                    barrier,
                    inc=1,
                    device_id=(section + 1, col_peer(step) * minor + b),
                    device_id_type=MESH,
                )

        expected = count - 1 + major * later + major * ((2 * sections - 2 - section) // sections)
        for distance in distances[1:]:
            partner = section + distance * (1 - 2 * ((section // distance) % 2))

            @pl.when(section % distance == 0)
            def _():
                pl.semaphore_signal(barrier, inc=1, device_id=(partner, me), device_id_type=MESH)

            expected += 1 - (section % distance + distance - 1) // distance
        pl.semaphore_wait(barrier, expected)

    def embed_copy(m, level):
        distance = distances[level]
        source = picked if level == 0 else emb_acc
        return remote(
            source.at[m],
            emb.at[level, m],
            emb_s.at[level, m],
            emb_r.at[level, m],
            (section - distance, me),
        )

    def embed_arrival(m, level):
        return remote(
            emb.at[level, m],
            emb.at[level, m],
            emb_s.at[level, m],
            emb_r.at[level, m],
            (section + distances[level], me),
        )

    def embed_tree(m):
        for level, distance in enumerate(distances):

            @pl.when(section % (2 * distance) == distance)
            def _():
                embed_copy(m, level).start()

            if level < len(distances) - 1:

                @pl.when(section % (2 * distance) == 0)
                def _():
                    embed_arrival(m, level).wait_recv()
                    source = picked if level == 0 else emb_acc
                    emb_acc[m] = source[m] + emb[level, m]

    def first_piece(m, chunk, side, sub):
        return xall.at[
            m, chunk, pl.ds(sub * minor, minor), :, pl.ds(pl.multiple_of(side * feats, feats), feats)
        ]

    def first_column(m, sub, step):
        piece = first_piece(m, a, b, sub)
        return remote(
            piece,
            piece,
            col_s.at[m, sub, step - 1],
            ag_r.at[m, a, sub * minor + b],
            peer(col_peer(step) * minor + b),
        )

    def first_forward(m, order, sub, step):
        chunk = col_peer(-order)
        piece = first_piece(m, chunk, b, sub)
        return remote(
            piece,
            piece,
            fwd_s.at[m, order, sub, step - 1],
            ag_r.at[m, chunk, sub * minor + b],
            peer(a * minor + row_peer(step)),
        )

    def embed_finish(m):
        level = len(distances) - 1
        embed_arrival(m, level).wait_recv()
        source = picked if level == 0 else emb_acc
        cols = pl.ds(pl.multiple_of(b * feats, feats), feats)
        xall[m, a, :, :, cols] = source[m] + emb[level, m]
        for sub in range(major):
            for step in range(1, minor):
                first_forward(m, 0, sub, step).start()
            for step in range(1, major):
                first_column(m, sub, step).start()

    @pl.when(section > 0)
    def _():
        for m in range(micros):
            embed_tree(m)

    with scope("p_wpeak"):
        act_out[...] = jnp.zeros_like(act_out)
        head_out[...] = jnp.zeros_like(head_out)
        positions = lax.broadcasted_iota(jnp.int32, (length, length), 0)
        keys_at = lax.broadcasted_iota(jnp.int32, (length, length), 1)
        causal = positions >= keys_at

        @pl.loop(0, width // LANES)
        def _(index):
            span_rows = pl.ds(pl.multiple_of(index * LANES, LANES), LANES)
            block = jnp.abs(wq[span_rows, :])
            peak = block[:, :LANES]
            for piece in range(1, query_cols // LANES):
                peak = jnp.maximum(peak, block[:, piece * LANES : (piece + 1) * LANES])
            turned = jnp.max(peak.astype(jnp.float32).T, axis=0, keepdims=True)
            keys = jnp.max(jnp.abs(wk[:, span_rows]).astype(jnp.float32), axis=0, keepdims=True)
            values = jnp.max(jnp.abs(wv[:, span_rows]).astype(jnp.float32), axis=0, keepdims=True)
            wpeak[:, span_rows] = jnp.maximum(turned, jnp.maximum(keys, values))

        for piece in range(query_cols // LANES):
            span_rows = pl.ds(piece * LANES, LANES)

            def widest(index, peak):
                cols = pl.ds(pl.multiple_of(index * TILE, TILE), TILE)
                block = jnp.abs(wo[span_rows, cols])
                for inner in range(TILE // LANES):
                    peak = jnp.maximum(peak, block[:, inner * LANES : (inner + 1) * LANES])
                return peak

            peak = lax.fori_loop(
                0, width // TILE, widest, jnp.zeros((LANES, LANES), jnp.bfloat16)
            )
            opeak_out[:, span_rows] = jnp.max(peak.astype(jnp.float32).T, axis=0, keepdims=True)

    @pl.when(section == 0)
    def _():
        embed_tree(0)
        embed_finish(0)
        for m in range(1, micros):
            embed_tree(m)

    def weight_copy(step):
        return remote(
            wpeak,
            wpbuf.at[me],
            wp_s.at[step - 1],
            wp_r.at[me],
            peer(lax.rem(me + step, count)),
        )

    def rotated(values):
        turned = pltpu.roll(values, HEAD_DIM // 2, 1)
        return (values * cos2[...] + turned * sin2[...]).astype(jnp.bfloat16)

    def tile_at(index):
        return pl.ds(pl.multiple_of(index * TILE, TILE), TILE)

    def forward(m, chunk, order, step):
        origin = col_peer(-order) * minor + b
        return remote(
            xall.at[m, chunk, origin],
            xall.at[m, chunk, origin],
            fwd_s.at[m, chunk, order, step - 1],
            ag_r.at[m, chunk, origin],
            peer(a * minor + row_peer(step)),
        )

    def onward(m, chunk, step):
        return remote(
            out.at[m, :, pl.ds(chunk * span, span)],
            xall.at[m, chunk, me],
            on_s.at[m, chunk, step],
            ag_r.at[m, chunk, me],
            (section + 1, col_peer(step) * minor + b),
        )

    def kv_copy(m, step):
        return remote(
            kvbuf.at[m, me],
            kvbuf.at[m, me],
            kv_s.at[m, step - 1],
            kv_r.at[m, me],
            peer(lax.rem(me + step, count)),
        )

    orders = list(range(1, major)) + [0]

    def first_copy(m, chunk, step, order):
        other_b = row_peer(step)
        other_a = col_peer(order)
        return remote(
            part.at[m, chunk, other_b, other_a],
            r1.at[m, chunk, b, other_a],
            r1_s.at[m, chunk, step - 1, order],
            r1_r.at[m, chunk, b, other_a],
            peer(a * minor + other_b),
        )

    def second_copy(m, chunk, order):
        return remote(
            s2.at[m, chunk, order - 1],
            r2.at[m, chunk, a],
            s2_s.at[m, chunk, order - 1],
            r2_r.at[m, chunk, a],
            peer(col_peer(order) * minor + b),
        )

    def micro_step(m):
        acc_q[...] = jnp.zeros_like(acc_q)
        acc_kv[...] = jnp.zeros_like(acc_kv)
        ssq[...] = jnp.zeros_like(ssq)

        def consume(chunk):
            @pl.loop(0, span // TILE)
            def _(index):
                cols = tile_at(index)
                full = pl.ds(pl.multiple_of(chunk * span + index * TILE, TILE), TILE)
                values = xall[m, chunk, :, :, cols].astype(jnp.float32).reshape(length, TILE)
                square = values * values
                total = square[:, :LANES]
                for piece in range(1, TILE // LANES):
                    total += square[:, piece * LANES : (piece + 1) * LANES]
                ssq[...] += total
                gained = (values * gain[:, full]).astype(jnp.bfloat16)
                acc_q[...] += jnp.dot(gained, wq[full, :], preferred_element_type=jnp.float32)
                wkv = jnp.concatenate([wk[:, full], wv[:, full]], axis=0)
                acc_kv[...] += lax.dot_general(
                    gained, wkv, (((1,), (1,)), ((), ())), preferred_element_type=jnp.float32
                )

        for turn in range(chunks + 1):
            if turn < chunks:
                with scope(f"p_col{turn}"):
                    if turn > 0:

                        @pl.when(section == 0)
                        def _():
                            chunk = col_peer(-turn)
                            for sub in range(major):
                                piece = first_piece(m, chunk, b, sub)
                                remote(
                                    piece,
                                    piece,
                                    fwd_s.at[m, turn, sub, 0],
                                    ag_r.at[m, chunk, sub * minor + b],
                                    peer(chunk * minor + b),
                                ).wait_recv()
                                for step in range(1, minor):
                                    first_forward(m, turn, sub, step).start()

                    @pl.when(section > 0)
                    def _():
                        for order in range(major):
                            origin = col_peer(-order) * minor + b
                            remote(
                                xall.at[m, turn, origin],
                                xall.at[m, turn, origin],
                                fwd_s.at[m, turn, order, 0],
                                ag_r.at[m, turn, origin],
                                (section - 1, origin),
                            ).wait_recv()
                            for step in range(1, minor):
                                forward(m, turn, order, step).start()

            if turn > 0:
                done = turn - 1
                with scope(f"p_row{done}"):

                    @pl.when(section == 0)
                    def _():
                        chunk = col_peer(-done)
                        for sub in range(major):
                            for step in range(1, minor):
                                side = row_peer(step)
                                piece = first_piece(m, chunk, side, sub)
                                remote(
                                    piece,
                                    piece,
                                    fwd_s.at[m, done, sub, step - 1],
                                    ag_r.at[m, chunk, sub * minor + side],
                                    peer(a * minor + side),
                                ).wait_recv()

                    @pl.when(section > 0)
                    def _():
                        for order in range(major):
                            for step in range(1, minor):
                                side = row_peer(step)
                                origin = col_peer(-order) * minor + side
                                remote(
                                    xall.at[m, done, origin],
                                    xall.at[m, done, origin],
                                    fwd_s.at[m, done, order, step - 1],
                                    ag_r.at[m, done, origin],
                                    peer(a * minor + side),
                                ).wait_recv()

                with scope(f"p_qkv{done}"):
                    consume(done * later + (1 - later) * col_peer(-done))

        with scope("p_scale"):
            inverse = lax.rsqrt(jnp.sum(ssq[...], axis=1, keepdims=True) / width + norm_eps)
            kvbuf[m, me] = (acc_kv[...] * inverse).astype(jnp.bfloat16)
            for step in range(1, count):
                kv_copy(m, step).start()

            @pl.when(jnp.logical_and(section == 0, m < micros - 1))
            def _():
                embed_finish(m + 1)

            queries = [
                rotated(acc_q[:, head * HEAD_DIM : (head + 1) * HEAD_DIM] * inverse)
                for head in range(heads_here)
            ]

        with scope("p_actpeak"):
            for chunk in range(chunks):

                @pl.loop(0, span // TILE)
                def _(index):
                    cols = tile_at(index)
                    full = pl.ds(pl.multiple_of(chunk * span + index * TILE, TILE), TILE)
                    values = xall[m, chunk, :, :, cols].astype(jnp.float32).reshape(length, TILE)
                    peak = jnp.max(jnp.abs(values * inverse), axis=0, keepdims=True)
                    peak = (peak * jnp.abs(gain[:, full])).astype(jnp.bfloat16)
                    act_out[:, full] = jnp.maximum(act_out[:, full], peak.astype(jnp.float32))

        with scope("p_kvwait"):
            for step in range(1, count):
                origin = lax.rem(me - step + count, count)
                remote(
                    kvbuf.at[m, origin],
                    kvbuf.at[m, origin],
                    kv_s.at[m, step - 1],
                    kv_r.at[m, origin],
                    peer(origin),
                ).wait_recv()
        with scope("p_attn"):
            for group in range(KV_HEADS):
                blocks = [
                    kvbuf[m, group * per_head + piece].astype(jnp.float32)
                    for piece in range(per_head)
                ]
                key = jnp.concatenate([block[:, :kv_cols] for block in blocks], axis=1)
                value = jnp.concatenate([block[:, kv_cols:] for block in blocks], axis=1)
                krot[group] = rotated(key)
                vall[group] = value.astype(jnp.bfloat16)
            for head in range(heads_here):
                if heads_here % KV_HEADS == 0:
                    group = head % KV_HEADS
                else:
                    group = lax.rem(me * heads_here + head, KV_HEADS)
                scores = lax.dot_general(
                    queries[head],
                    krot[group],
                    (((1,), (1,)), ((), ())),
                    preferred_element_type=jnp.float32,
                ) / math.sqrt(HEAD_DIM)
                scores = jnp.where(causal, scores, -1e30)
                weights = jnp.exp(scores - jnp.max(scores, axis=1, keepdims=True))
                probs = (weights / jnp.sum(weights, axis=1, keepdims=True)).astype(jnp.bfloat16)
                mixed = jnp.dot(probs, vall[group], preferred_element_type=jnp.float32)
                mixed = mixed.astype(jnp.bfloat16)
                cols = pl.ds(head * HEAD_DIM, HEAD_DIM)
                att[:, cols] = mixed
                peak = jnp.max(jnp.abs(mixed.astype(jnp.float32)), axis=0, keepdims=True)
                head_out[:, cols] = jnp.maximum(head_out[:, cols], peak)

        with scope("p_oproj"):
            for chunk in range(chunks):

                @pl.loop(0, span // TILE)
                def _(index):
                    cols = tile_at(index)
                    source = tile_at(index + chunk * (span // TILE))
                    product = jnp.dot(att[...], wo[:, source], preferred_element_type=jnp.float32)
                    for i in range(major):
                        for j in range(minor):
                            top = (i * minor + j) * rows
                            part[m, chunk, j, i, :, cols] = product[top : top + rows].astype(
                                jnp.bfloat16
                            )

                for order in orders:
                    for step in range(1, minor):
                        first_copy(m, chunk, step, order).start()

        def first_sum(chunk):
            for order in orders:
                other_a = col_peer(order)
                for step in range(1, minor):
                    origin = row_peer(step)
                    remote(
                        r1.at[m, chunk, origin, other_a],
                        r1.at[m, chunk, origin, other_a],
                        r1_s.at[m, chunk, step - 1, order],
                        r1_r.at[m, chunk, origin, other_a],
                        peer(a * minor + origin),
                    ).wait_recv()
                for index in range(span // TILE):
                    cols = pl.ds(index * TILE, TILE)
                    total = part[m, chunk, b, other_a, :, cols].astype(jnp.float32)
                    for step in range(1, minor):
                        total += r1[m, chunk, row_peer(step), other_a, :, cols].astype(jnp.float32)
                    if order == 0:
                        own[chunk, :, cols] = total
                    else:
                        s2[m, chunk, order - 1, :, cols] = total.astype(jnp.bfloat16)
                if order != 0:
                    second_copy(m, chunk, order).start()

        def second_sum(chunk):
            for order in range(1, major):
                origin = col_peer(-order)
                remote(
                    r2.at[m, chunk, origin],
                    r2.at[m, chunk, origin],
                    s2_s.at[m, chunk, order - 1],
                    r2_r.at[m, chunk, origin],
                    peer(origin * minor + b),
                ).wait_recv()
            for index in range(span // TILE):
                cols = pl.ds(index * TILE, TILE)
                full = pl.ds(chunk * span + index * TILE, TILE)
                total = own[chunk, :, cols]
                for order in range(1, major):
                    total += r2[m, chunk, col_peer(-order), :, cols].astype(jnp.float32)
                rest = xall[m, chunk, me, :, cols].astype(jnp.float32)
                out[m, :, full] = (rest + total).astype(jnp.bfloat16)

            @pl.when(section < sections - 1)
            def _():
                for step in range(major):
                    onward(m, chunk, step).start()

        for chunk in range(chunks + 1):
            if chunk < chunks:
                with scope(f"p_rs1_{chunk}"):
                    first_sum(chunk)
            if chunk > 0:
                with scope(f"p_rs2_{chunk - 1}"):
                    second_sum(chunk - 1)

        @pl.when(m == 0)
        def _():
            for step in range(1, count):
                weight_copy(step).start()

    @pl.loop(0, micros)
    def _(m):
        micro_step(m)

    with scope("p_wpwait"):
        peak = wpeak[...]
        for step in range(1, count):
            origin = lax.rem(me + step, count)
            remote(
                wpeak, wpbuf.at[origin], wp_s.at[step - 1], wp_r.at[origin], peer(origin)
            ).wait_recv()
            peak = jnp.maximum(peak, wpbuf[origin])
        wpeak_out[...] = peak

    with scope("p_sends"):
        for level, distance in enumerate(distances):

            @pl.when(section % (2 * distance) == distance)
            def _():
                for m in range(micros):
                    embed_copy(m, level).wait_send()

        for m in range(micros):

            @pl.when(section == 0)
            def _():
                for sub in range(major):
                    for step in range(1, major):
                        first_column(m, sub, step).wait_send()
                for order in range(major):
                    for sub in range(major):
                        for step in range(1, minor):
                            first_forward(m, order, sub, step).wait_send()

            @pl.when(section > 0)
            def _():
                for chunk in range(chunks):
                    for order in range(major):
                        for step in range(1, minor):
                            forward(m, chunk, order, step).wait_send()

            @pl.when(section < sections - 1)
            def _():
                for chunk in range(chunks):
                    for step in range(major):
                        onward(m, chunk, step).wait_send()

            for step in range(1, count):
                kv_copy(m, step).wait_send()
            for chunk in range(chunks):
                for order in orders:
                    for step in range(1, minor):
                        first_copy(m, chunk, step, order).wait_send()
                    if order != 0:
                        second_copy(m, chunk, order).wait_send()
        for step in range(1, count):
            weight_copy(step).wait_send()


def run_layers(sections, count, picked, gain, wq, wk, wv, wo, cos2, sin2):
    major, minor = grid_of(count)
    micros, _, rows, feats = picked.shape
    width = feats * count
    length = rows * count
    query_cols = wq.shape[1]
    kv_two = 2 * wk.shape[0]
    levels = len(levels_of(sections))
    chunks = major
    span = width // chunks
    bf16, f32 = jnp.bfloat16, jnp.float32
    vmem = pl.BlockSpec(memory_space=pltpu.VMEM)
    dma = pltpu.SemaphoreType.DMA
    return pl.pallas_call(
        functools.partial(layers_kernel, sections, count),
        out_shape=(
            jax.ShapeDtypeStruct((micros, rows, width), bf16),
            jax.ShapeDtypeStruct((1, width), f32),
            jax.ShapeDtypeStruct((1, query_cols), f32),
            jax.ShapeDtypeStruct((1, width), f32),
            jax.ShapeDtypeStruct((1, query_cols), f32),
        ),
        in_specs=[vmem] * 8,
        out_specs=(vmem,) * 5,
        scratch_shapes=[
            pltpu.VMEM((levels, micros, count, rows, feats), bf16),
            pltpu.VMEM((micros, count, rows, feats), bf16),
            pltpu.VMEM((micros, chunks, count, rows, span), bf16),
            pltpu.VMEM((length, LANES), f32),
            pltpu.VMEM((length, query_cols), f32),
            pltpu.VMEM((length, kv_two), f32),
            pltpu.VMEM((micros, count, length, kv_two), bf16),
            pltpu.VMEM((KV_HEADS, length, HEAD_DIM), bf16),
            pltpu.VMEM((KV_HEADS, length, HEAD_DIM), bf16),
            pltpu.VMEM((length, query_cols), bf16),
            pltpu.VMEM((micros, chunks, minor, major, rows, span), bf16),
            pltpu.VMEM((micros, chunks, minor, major, rows, span), bf16),
            pltpu.VMEM((micros, chunks, major - 1, rows, span), bf16),
            pltpu.VMEM((micros, chunks, major, rows, span), bf16),
            pltpu.VMEM((chunks, rows, span), f32),
            pltpu.VMEM((1, width), f32),
            pltpu.VMEM((count, 1, width), f32),
            dma((levels, micros)),
            dma((levels, micros)),
            dma((micros, major, major - 1)),
            dma((micros, chunks, major, minor - 1)),
            dma((micros, chunks, major)),
            dma((micros, chunks, count)),
            dma((micros, count - 1)),
            dma((micros, count)),
            dma((micros, chunks, minor - 1, major)),
            dma((micros, chunks, minor, major)),
            dma((micros, chunks, major - 1)),
            dma((micros, chunks, major)),
            dma((count - 1,)),
            dma((count,)),
        ],
        compiler_params=pltpu.CompilerParams(
            collective_id=0, has_side_effects=True, vmem_limit_bytes=VMEM_MIB * 1024 * 1024
        ),
        name="layers",
    )(picked, gain, wq, wk, wv, wo, cos2, sin2)


VMEM_MIB = 24


def shards(token_ids, alpha_num, embed_table, norm_gain, w_query, w_key, w_value, w_out):
    tp_count = lax.axis_size("tp")
    section_count = lax.axis_size("section")
    section_index = lax.axis_index("section")
    micros, length = token_ids.shape
    vocab_rows, feats = embed_table.shape
    local_ids = token_ids - section_index * vocab_rows
    inside = (local_ids >= 0) & (local_ids < vocab_rows)
    picked = jnp.take(embed_table, jnp.clip(local_ids, 0, vocab_rows - 1), axis=0)
    picked = jnp.where(inside[:, :, None], picked, jnp.zeros_like(picked))
    picked = picked.reshape(micros, tp_count, length // tp_count, feats)
    w_query, w_key, w_value, w_out = w_query[0], w_key[0], w_value[0], w_out[0]
    cosine, sine = rope_tables(length, HEAD_DIM)
    cos2 = jnp.concatenate([cosine, cosine], axis=1)
    sin2 = jnp.concatenate([-sine, sine], axis=1)
    stored, act_peak, head_peak, weight_peak, out_peak = run_layers(
        section_count,
        tp_count,
        picked,
        norm_gain,
        w_query,
        w_key.T,
        w_value.T,
        w_out,
        cos2,
        sin2,
    )
    alpha_exp = alpha_num[0].astype(jnp.float32) / 10.0
    scale_in = smoothing(act_peak[0], weight_peak[0], alpha_exp)
    scale_out = smoothing(head_peak[0], out_peak[0], alpha_exp)

    def smoothed(weights):
        return (weights.astype(jnp.float32) * scale_in[:, None]).astype(jnp.bfloat16)

    return (
        stored[None],
        scale_in[None],
        scale_out[None],
        smoothed(w_query)[None],
        smoothed(w_key)[None],
        smoothed(w_value)[None],
    )


def solution(mesh):
    return jax.shard_map(
        shards,
        mesh=mesh,
        in_specs=(
            P(),
            P(),
            P("section", "tp"),
            P("section", None),
            P("section", None, "tp"),
            P("section", None, "tp"),
            P("section", None, "tp"),
            P("section", "tp", None),
        ),
        out_specs=(
            P("section", None, "tp", None),
            P("section", None),
            P("section", "tp"),
            P("section", None, "tp"),
            P("section", None, "tp"),
            P("section", None, "tp"),
        ),
        check_vma=False,
    )
```

```python
import contextlib
import functools
import math

import jax
import jax.numpy as jnp
from jax import lax
from jax.experimental import pallas as pl
from jax.experimental.pallas import tpu as pltpu
from jax.sharding import PartitionSpec as P

KV_HEADS = 4
HEAD_DIM = 128


norm_eps = 1e-05
stat_eps = 1e-05
rope_base = 500000.0


def rope_tables(length, head_size):
    halves = head_size // 2
    freqs = jnp.exp(-math.log(rope_base) * 2.0 * jnp.arange(halves, dtype=jnp.float32) / head_size)
    angles = jnp.arange(length, dtype=jnp.float32)[:, None] * freqs[None, :]
    return (jnp.cos(angles), jnp.sin(angles))


def smoothing(act_peak, weight_peak, alpha_exp):
    return jnp.exp(
        alpha_exp * jnp.log(act_peak + stat_eps)
        - (1.0 - alpha_exp) * jnp.log(weight_peak + stat_eps)
    )


MESH = pl.DeviceIdType.MESH
TILE = 512
LANES = 128


def scope(name):
    return contextlib.nullcontext()


def remote(src, dst, send, recv, where):
    return pltpu.make_async_remote_copy(
        src_ref=src, dst_ref=dst, send_sem=send, recv_sem=recv, device_id=where, device_id_type=MESH
    )


def grid_of(count):
    minor = 1
    while (2 * minor) * (2 * minor) <= count and count % (2 * minor) == 0:
        minor *= 2
    return (count // minor, minor)


def levels_of(sections):
    distances = []
    while (1 << len(distances)) < sections:
        distances.append(1 << len(distances))
    return distances


def layers_kernel(
    sections,
    count,
    picked,
    gain,
    wq_hbm,
    wk_hbm,
    wv_hbm,
    wo_hbm,
    cos2,
    sin2,
    alpha,
    out,
    scale_in,
    scale_out,
    wq,
    wk,
    wv,
    wo,
    act_peak,
    head_peak,
    opeak,
    qrot,
    emb,
    emb_acc,
    xall,
    ssq,
    acc_q,
    acc_kv,
    kvbuf,
    krot,
    vall,
    att,
    part,
    r1,
    s2,
    r2,
    own,
    wpeak,
    wpbuf,
    load_sem,
    emb_s,
    emb_r,
    col_s,
    fwd_s,
    on_s,
    ag_r,
    kv_s,
    kv_r,
    r1_s,
    r1_r,
    s2_s,
    r2_r,
    wp_s,
    wp_r,
    gate,
):
    major, minor = grid_of(count)
    section = lax.axis_index("section")
    me = lax.axis_index("tp")
    a = me // minor
    b = me % minor
    micros, _, rows, feats = picked.shape
    width = feats * count
    length = rows * count
    query_cols = wq.shape[1]
    kv_cols = wk.shape[0]
    heads_here = query_cols // HEAD_DIM
    per_head = HEAD_DIM // kv_cols
    chunks = major
    span = width // chunks
    distances = levels_of(sections)
    later = (section + sections - 1) // sections

    def peer(number):
        return (section, number)

    def col_peer(step):
        return lax.rem(a + step + major, major)

    def row_peer(step):
        return lax.rem(b + step + minor, minor)

    loads = [
        pltpu.make_async_copy(wq_hbm, wq, load_sem.at[0]),
        pltpu.make_async_copy(wk_hbm, wk, load_sem.at[1]),
        pltpu.make_async_copy(wv_hbm, wv, load_sem.at[2]),
        pltpu.make_async_copy(wo_hbm, wo, load_sem.at[3]),
    ]
    for load in loads:
        load.start()

    with scope("p_barrier"):
        barrier = pltpu.get_barrier_semaphore()
        for step in range(1, count):
            pl.semaphore_signal(
                barrier, inc=1, device_id=peer(lax.rem(me + step, count)), device_id_type=MESH
            )

        @pl.when(section > 0)
        def _():
            for step in range(major):
                pl.semaphore_signal(
                    barrier,
                    inc=1,
                    device_id=(section - 1, col_peer(step) * minor + b),
                    device_id_type=MESH,
                )

        @pl.when(section < sections - 1)
        def _():
            for step in range(major):
                pl.semaphore_signal(
                    barrier,
                    inc=1,
                    device_id=(section + 1, col_peer(step) * minor + b),
                    device_id_type=MESH,
                )

        expected = count - 1 + major * later + major * ((2 * sections - 2 - section) // sections)
        for distance in distances[1:]:
            partner = section + distance * (1 - 2 * ((section // distance) % 2))

            @pl.when(section % distance == 0)
            def _():
                pl.semaphore_signal(barrier, inc=1, device_id=(partner, me), device_id_type=MESH)

            expected += 1 - (section % distance + distance - 1) // distance
        pl.semaphore_wait(barrier, expected)

    def embed_copy(m, level):
        distance = distances[level]
        source = picked if level == 0 else emb_acc
        return remote(
            source.at[m],
            emb.at[level, m],
            emb_s.at[level, m],
            emb_r.at[level, m],
            (section - distance, me),
        )

    def embed_arrival(m, level):
        return remote(
            emb.at[level, m],
            emb.at[level, m],
            emb_s.at[level, m],
            emb_r.at[level, m],
            (section + distances[level], me),
        )

    def embed_tree(m):
        for level, distance in enumerate(distances):

            @pl.when(section % (2 * distance) == distance)
            def _():
                embed_copy(m, level).start()

            if level < len(distances) - 1:

                @pl.when(section % (2 * distance) == 0)
                def _():
                    embed_arrival(m, level).wait_recv()
                    source = picked if level == 0 else emb_acc
                    emb_acc[m] = source[m] + emb[level, m]

    def first_piece(m, chunk, side, sub):
        return xall.at[
            m, chunk, pl.ds(sub * minor, minor), :, pl.ds(pl.multiple_of(side * feats, feats), feats)
        ]

    def first_column(m, sub, step):
        piece = first_piece(m, a, b, sub)
        return remote(
            piece,
            piece,
            col_s.at[m, sub, step - 1],
            ag_r.at[m, a, sub * minor + b],
            peer(col_peer(step) * minor + b),
        )

    def first_forward(m, order, sub, step):
        chunk = col_peer(-order)
        piece = first_piece(m, chunk, b, sub)
        return remote(
            piece,
            piece,
            fwd_s.at[m, order, sub, step - 1],
            ag_r.at[m, chunk, sub * minor + b],
            peer(a * minor + row_peer(step)),
        )

    def embed_finish(m):
        level = len(distances) - 1
        embed_arrival(m, level).wait_recv()
        source = picked if level == 0 else emb_acc
        cols = pl.ds(pl.multiple_of(b * feats, feats), feats)
        xall[m, a, :, :, cols] = source[m] + emb[level, m]
        for sub in range(major):
            for step in range(1, minor):
                first_forward(m, 0, sub, step).start()
            for step in range(1, major):
                first_column(m, sub, step).start()

    act_peak[...] = jnp.zeros_like(act_peak)
    head_peak[...] = jnp.zeros_like(head_peak)
    positions = lax.broadcasted_iota(jnp.int32, (length, length), 0)
    keys_at = lax.broadcasted_iota(jnp.int32, (length, length), 1)
    causal = positions >= keys_at

    def weight_peaks():
        @pl.loop(0, width // LANES)
        def _(index):
            span_rows = pl.ds(pl.multiple_of(index * LANES, LANES), LANES)
            block = jnp.abs(wq[span_rows, :])
            peak = block[:, :LANES]
            for piece in range(1, query_cols // LANES):
                peak = jnp.maximum(peak, block[:, piece * LANES : (piece + 1) * LANES])
            turned = jnp.max(peak.astype(jnp.float32).T, axis=0, keepdims=True)
            keys = jnp.max(jnp.abs(wk[:, span_rows]).astype(jnp.float32), axis=0, keepdims=True)
            values = jnp.max(jnp.abs(wv[:, span_rows]).astype(jnp.float32), axis=0, keepdims=True)
            wpeak[:, span_rows] = jnp.maximum(turned, jnp.maximum(keys, values))

        for piece in range(query_cols // LANES):
            span_rows = pl.ds(piece * LANES, LANES)

            def widest(index, peak):
                cols = pl.ds(pl.multiple_of(index * TILE, TILE), TILE)
                block = jnp.abs(wo[span_rows, cols])
                for inner in range(TILE // LANES):
                    peak = jnp.maximum(peak, block[:, inner * LANES : (inner + 1) * LANES])
                return peak

            peak = lax.fori_loop(
                0, width // TILE, widest, jnp.zeros((LANES, LANES), jnp.bfloat16)
            )
            opeak[:, span_rows] = jnp.max(peak.astype(jnp.float32).T, axis=0, keepdims=True)

    with scope("p_embed"):

        @pl.when(section > 0)
        def _():
            for m in range(micros):
                embed_tree(m)

        @pl.when(section == 0)
        def _():
            embed_tree(0)
            embed_finish(0)
            for m in range(1, micros):
                embed_tree(m)

    with scope("p_load"):
        for load in loads:
            load.wait()

    with scope("p_wpeak"):

        @pl.when(section > 0)
        def _():
            weight_peaks()

    def weight_copy(step):
        return remote(
            wpeak,
            wpbuf.at[me],
            wp_s.at[step - 1],
            wp_r.at[me],
            peer(lax.rem(me + step, count)),
        )

    def rotated(values):
        turned = pltpu.roll(values, HEAD_DIM // 2, 1)
        return (values * cos2[...] + turned * sin2[...]).astype(jnp.bfloat16)

    def tile_at(index):
        return pl.ds(pl.multiple_of(index * TILE, TILE), TILE)

    def forward(m, chunk, order, step):
        origin = col_peer(-order) * minor + b
        return remote(
            xall.at[m, chunk, origin],
            xall.at[m, chunk, origin],
            fwd_s.at[m, chunk, order, step - 1],
            ag_r.at[m, chunk, origin],
            peer(a * minor + row_peer(step)),
        )

    def onward(m, chunk, step):
        return remote(
            out.at[m, :, pl.ds(chunk * span, span)],
            xall.at[m, chunk, me],
            on_s.at[m, chunk, step],
            ag_r.at[m, chunk, me],
            (section + 1, col_peer(step) * minor + b),
        )

    def spread(m, chunk, step):
        return remote(
            xall.at[m, chunk, me],
            xall.at[m, chunk, me],
            col_s.at[m, chunk, step - 1],
            ag_r.at[m, chunk, me],
            peer(col_peer(step) * minor + b),
        )

    def kv_copy(m, step):
        return remote(
            kvbuf.at[m, me],
            kvbuf.at[m, me],
            kv_s.at[m, step - 1],
            kv_r.at[m, me],
            peer(lax.rem(me + step, count)),
        )

    orders = list(range(1, major)) + [0]

    def first_copy(m, chunk, step, order):
        other_b = row_peer(step)
        other_a = col_peer(order)
        return remote(
            part.at[m, chunk, other_b, other_a],
            r1.at[m, chunk, b, other_a],
            r1_s.at[m, chunk, step - 1, order],
            r1_r.at[m, chunk, b, other_a],
            peer(a * minor + other_b),
        )

    def second_copy(m, chunk, order):
        return remote(
            s2.at[m, chunk, order - 1],
            r2.at[m, chunk, a],
            s2_s.at[m, chunk, order - 1],
            r2_r.at[m, chunk, a],
            peer(col_peer(order) * minor + b),
        )

    def consume(m, chunk):
        @pl.loop(0, span // TILE)
        def _(index):
            cols = tile_at(index)
            full = pl.ds(pl.multiple_of(chunk * span + index * TILE, TILE), TILE)
            values = xall[m, chunk, :, :, cols].astype(jnp.float32).reshape(length, TILE)
            square = values * values
            total = square[:, :LANES]
            for piece in range(1, TILE // LANES):
                total += square[:, piece * LANES : (piece + 1) * LANES]
            ssq[...] += total
            gained = (values * gain[:, full]).astype(jnp.bfloat16)
            acc_q[...] += jnp.dot(gained, wq[full, :], preferred_element_type=jnp.float32)
            wkv = jnp.concatenate([wk[:, full], wv[:, full]], axis=0)
            acc_kv[...] += lax.dot_general(
                gained, wkv, (((1,), (1,)), ((), ())), preferred_element_type=jnp.float32
            )

    def first_cols(m, turn):
        chunk = col_peer(-turn)
        for sub in range(major):
            piece = first_piece(m, chunk, b, sub)
            remote(
                piece,
                piece,
                fwd_s.at[m, turn, sub, 0],
                ag_r.at[m, chunk, sub * minor + b],
                peer(chunk * minor + b),
            ).wait_recv()
            for step in range(1, minor):
                first_forward(m, turn, sub, step).start()

    def first_rows(m, turn):
        chunk = col_peer(-turn)
        for sub in range(major):
            for step in range(1, minor):
                side = row_peer(step)
                piece = first_piece(m, chunk, side, sub)
                remote(
                    piece,
                    piece,
                    fwd_s.at[m, turn, sub, step - 1],
                    ag_r.at[m, chunk, sub * minor + side],
                    peer(a * minor + side),
                ).wait_recv()

    def next_col(m, chunk, order):
        origin = col_peer(-order) * minor + b
        remote(
            xall.at[m, chunk, origin],
            xall.at[m, chunk, origin],
            fwd_s.at[m, chunk, order, 0],
            ag_r.at[m, chunk, origin],
            (section - 1, origin),
        ).wait_recv()
        for step in range(1, minor):
            forward(m, chunk, order, step).start()

    def next_own(m, chunk):
        next_col(m, chunk, 0)

        @pl.when(section % 2 == 0)
        def _():
            for step in range(1, major):
                spread(m, chunk, step).start()

    def next_cols(m, chunk):
        if chunk == 0:
            next_own(m, 0)
        if chunk < chunks - 1:
            next_own(m, chunk + 1)
        for order in range(1, major):
            next_col(m, chunk, order)

    def next_rows(m, chunk):
        for order in range(major):
            for step in range(1, minor):
                side = row_peer(step)
                origin = col_peer(-order) * minor + side
                remote(
                    xall.at[m, chunk, origin],
                    xall.at[m, chunk, origin],
                    fwd_s.at[m, chunk, order, step - 1],
                    ag_r.at[m, chunk, origin],
                    peer(a * minor + side),
                ).wait_recv()

    def clear():
        acc_q[...] = jnp.zeros_like(acc_q)
        acc_kv[...] = jnp.zeros_like(acc_kv)
        ssq[...] = jnp.zeros_like(ssq)

    def inverse_norm():
        return lax.rsqrt(jnp.sum(ssq[...], axis=1, keepdims=True) / width + norm_eps)

    def project(m):
        inverse = inverse_norm()
        kvbuf[m, me] = (acc_kv[...] * inverse).astype(jnp.bfloat16)
        for step in range(1, count):
            kv_copy(m, step).start()

        for head in range(heads_here):
            qrot[head] = rotated(acc_q[:, head * HEAD_DIM : (head + 1) * HEAD_DIM] * inverse)

    clear()
    for turn in range(chunks + 1):
        if turn < chunks:
            with scope(f"p_col{turn}"):
                if turn > 0:

                    @pl.when(section == 0)
                    def _():
                        first_cols(0, turn)

                @pl.when(section > 0)
                def _():
                    next_cols(0, turn)

        if turn > 0:
            done = turn - 1
            with scope(f"p_row{done}"):

                @pl.when(section == 0)
                def _():
                    first_rows(0, done)

                @pl.when(section > 0)
                def _():
                    next_rows(0, done)

            with scope(f"p_qkv{done}"):
                consume(0, done * later + (1 - later) * col_peer(-done))
    with scope("p_project"):
        project(0)

    def micro_step(m):
        more = m < micros - 1
        with scope("p_actpeak"):
            inverse = inverse_norm()

            @pl.loop(0, width // TILE)
            def _(index):
                full = tile_at(index)
                chunk = index // (span // TILE)
                cols = tile_at(index % (span // TILE))
                values = xall[m, chunk, :, :, cols].astype(jnp.float32).reshape(length, TILE)
                peak = jnp.max(jnp.abs(values * inverse), axis=0, keepdims=True)
                peak = (peak * jnp.abs(gain[:, full])).astype(jnp.bfloat16)
                act_peak[:, full] = jnp.maximum(act_peak[:, full], peak.astype(jnp.float32))

        with scope("p_kvwait"):
            for step in range(1, count):
                origin = lax.rem(me - step + count, count)
                remote(
                    kvbuf.at[m, origin],
                    kvbuf.at[m, origin],
                    kv_s.at[m, step - 1],
                    kv_r.at[m, origin],
                    peer(origin),
                ).wait_recv()

        @pl.when(jnp.logical_and(more, section == 0))
        def _():
            embed_finish(m + 1)

        with scope("p_attn"):
            for group in range(KV_HEADS):
                blocks = [
                    kvbuf[m, group * per_head + piece].astype(jnp.float32)
                    for piece in range(per_head)
                ]
                key = jnp.concatenate([block[:, :kv_cols] for block in blocks], axis=1)
                value = jnp.concatenate([block[:, kv_cols:] for block in blocks], axis=1)
                krot[group] = rotated(key)
                vall[group] = value.astype(jnp.bfloat16)
            for head in range(heads_here):
                if heads_here % KV_HEADS == 0:
                    group = head % KV_HEADS
                else:
                    group = lax.rem(me * heads_here + head, KV_HEADS)
                scores = lax.dot_general(
                    qrot[head],
                    krot[group],
                    (((1,), (1,)), ((), ())),
                    preferred_element_type=jnp.float32,
                ) / math.sqrt(HEAD_DIM)
                scores = jnp.where(causal, scores, -1e30)
                weights = jnp.exp(scores - jnp.max(scores, axis=1, keepdims=True))
                probs = (weights / jnp.sum(weights, axis=1, keepdims=True)).astype(jnp.bfloat16)
                mixed = jnp.dot(probs, vall[group], preferred_element_type=jnp.float32)
                mixed = mixed.astype(jnp.bfloat16)
                cols = pl.ds(head * HEAD_DIM, HEAD_DIM)
                att[:, cols] = mixed
                peak = jnp.max(jnp.abs(mixed.astype(jnp.float32)), axis=0, keepdims=True)
                head_peak[:, cols] = jnp.maximum(head_peak[:, cols], peak)

        with scope("p_gate"):

            @pl.when(jnp.logical_and(m > 0, section % 2 == 0))
            def _():
                pl.semaphore_wait(gate, 1)

        with scope("p_oproj"):
            for chunk in range(chunks):

                @pl.loop(0, span // TILE)
                def _(index):
                    cols = tile_at(index)
                    source = tile_at(index + chunk * (span // TILE))
                    product = jnp.dot(att[...], wo[:, source], preferred_element_type=jnp.float32)
                    for i in range(major):
                        for j in range(minor):
                            top = (i * minor + j) * rows
                            part[m, chunk, j, i, :, cols] = product[top : top + rows].astype(
                                jnp.bfloat16
                            )

                for order in orders:
                    for step in range(1, minor):
                        first_copy(m, chunk, step, order).start()

        def first_sum(chunk):
            for order in orders:
                other_a = col_peer(order)
                for step in range(1, minor):
                    origin = row_peer(step)
                    remote(
                        r1.at[m, chunk, origin, other_a],
                        r1.at[m, chunk, origin, other_a],
                        r1_s.at[m, chunk, step - 1, order],
                        r1_r.at[m, chunk, origin, other_a],
                        peer(a * minor + origin),
                    ).wait_recv()
                for index in range(span // TILE):
                    cols = pl.ds(index * TILE, TILE)
                    total = part[m, chunk, b, other_a, :, cols].astype(jnp.float32)
                    for step in range(1, minor):
                        total += r1[m, chunk, row_peer(step), other_a, :, cols].astype(jnp.float32)
                    if order == 0:
                        own[chunk, :, cols] = total
                    else:
                        s2[m, chunk, order - 1, :, cols] = total.astype(jnp.bfloat16)
                if order != 0:
                    second_copy(m, chunk, order).start()

        def second_sum(chunk):
            for order in range(1, major):
                origin = col_peer(-order)
                remote(
                    r2.at[m, chunk, origin],
                    r2.at[m, chunk, origin],
                    s2_s.at[m, chunk, order - 1],
                    r2_r.at[m, chunk, origin],
                    peer(origin * minor + b),
                ).wait_recv()
            for index in range(span // TILE):
                cols = pl.ds(index * TILE, TILE)
                full = pl.ds(chunk * span + index * TILE, TILE)
                total = own[chunk, :, cols]
                for order in range(1, major):
                    total += r2[m, chunk, col_peer(-order), :, cols].astype(jnp.float32)
                rest = xall[m, chunk, me, :, cols].astype(jnp.float32)
                out[m, :, full] = (rest + total).astype(jnp.bfloat16)

            @pl.when(section < sections - 1)
            def _():
                onward(m, chunk, 0).start()

            @pl.when(jnp.logical_and(section < sections - 1, section % 2 == 0))
            def _():
                for step in range(1, major):
                    onward(m, chunk, step).start()

        @pl.when(more)
        def _():
            clear()

        @pl.when(jnp.logical_and(more, section == 0))
        def _():
            for turn in range(1, major):
                first_cols(m + 1, turn)

        for chunk in range(chunks + 1):
            if chunk < chunks:
                with scope(f"p_rs1_{chunk}"):
                    first_sum(chunk)
            if chunk == 1:

                @pl.when(jnp.logical_and(more, section % 2 == 1))
                def _():
                    pl.semaphore_signal(
                        gate, inc=1, device_id=(section - 1, me), device_id_type=MESH
                    )

            if chunk > 0:
                with scope(f"p_rs2_{chunk - 1}"):
                    second_sum(chunk - 1)

        with scope("p_nextfirst"):

            @pl.when(jnp.logical_and(more, section == 0))
            def _():
                @pl.loop(0, major)
                def _(turn):
                    first_rows(m + 1, turn)
                    consume(m + 1, col_peer(-turn))

        for turn in range(chunks + 1):
            with scope(f"p_next{turn}"):

                @pl.when(jnp.logical_and(more, section > 0))
                def _():
                    if turn < chunks:
                        next_cols(m + 1, turn)
                    if turn > 0:
                        next_rows(m + 1, turn - 1)
                        consume(m + 1, turn - 1)

        with scope("p_project"):

            @pl.when(more)
            def _():
                project(m + 1)

        @pl.when(jnp.logical_and(m == 0, section > 0))
        def _():
            for step in range(1, count):
                weight_copy(step).start()

    @pl.loop(0, micros)
    def _(m):
        micro_step(m)

    @pl.when(section == 0)
    def _():
        weight_peaks()
        for step in range(1, count):
            weight_copy(step).start()

    with scope("p_scales"):
        peak = wpeak[...]
        for step in range(1, count):
            origin = lax.rem(me + step, count)
            remote(
                wpeak, wpbuf.at[origin], wp_s.at[step - 1], wp_r.at[origin], peer(origin)
            ).wait_recv()
            peak = jnp.maximum(peak, wpbuf[origin])
        scale_in[...] = smoothing(act_peak[...], peak, alpha[...])
        scale_out[...] = smoothing(head_peak[...], opeak[...], alpha[...])

    with scope("p_sends"):
        for level, distance in enumerate(distances):

            @pl.when(section % (2 * distance) == distance)
            def _():
                for m in range(micros):
                    embed_copy(m, level).wait_send()

        for m in range(micros):

            @pl.when(section == 0)
            def _():
                for sub in range(major):
                    for step in range(1, major):
                        first_column(m, sub, step).wait_send()
                for order in range(major):
                    for sub in range(major):
                        for step in range(1, minor):
                            first_forward(m, order, sub, step).wait_send()

            @pl.when(section > 0)
            def _():
                for chunk in range(chunks):
                    for order in range(major):
                        for step in range(1, minor):
                            forward(m, chunk, order, step).wait_send()

            @pl.when(section < sections - 1)
            def _():
                for chunk in range(chunks):
                    onward(m, chunk, 0).wait_send()

            @pl.when(jnp.logical_and(section < sections - 1, section % 2 == 0))
            def _():
                for chunk in range(chunks):
                    for step in range(1, major):
                        onward(m, chunk, step).wait_send()

            @pl.when(jnp.logical_and(section > 0, section % 2 == 0))
            def _():
                for chunk in range(chunks):
                    for step in range(1, major):
                        spread(m, chunk, step).wait_send()

            for step in range(1, count):
                kv_copy(m, step).wait_send()
            for chunk in range(chunks):
                for order in orders:
                    for step in range(1, minor):
                        first_copy(m, chunk, step, order).wait_send()
                    if order != 0:
                        second_copy(m, chunk, order).wait_send()
        for step in range(1, count):
            weight_copy(step).wait_send()


def run_layers(sections, count, picked, gain, wq, wk, wv, wo, cos2, sin2, alpha):
    major, minor = grid_of(count)
    micros, _, rows, feats = picked.shape
    width = feats * count
    length = rows * count
    query_cols = wq.shape[1]
    kv_two = 2 * wk.shape[0]
    levels = len(levels_of(sections))
    chunks = major
    span = width // chunks
    bf16, f32 = jnp.bfloat16, jnp.float32
    vmem = pl.BlockSpec(memory_space=pltpu.VMEM)
    anywhere = pl.BlockSpec(memory_space=pltpu.HBM)
    dma = pltpu.SemaphoreType.DMA
    return pl.pallas_call(
        functools.partial(layers_kernel, sections, count),
        out_shape=(
            jax.ShapeDtypeStruct((micros, rows, width), bf16),
            jax.ShapeDtypeStruct((1, width), f32),
            jax.ShapeDtypeStruct((1, query_cols), f32),
        ),
        in_specs=[vmem] * 2 + [anywhere] * 4 + [vmem] * 3,
        out_specs=(vmem,) * 3,
        scratch_shapes=[
            pltpu.VMEM(wq.shape, bf16),
            pltpu.VMEM(wk.shape, bf16),
            pltpu.VMEM(wv.shape, bf16),
            pltpu.VMEM(wo.shape, bf16),
            pltpu.VMEM((1, width), f32),
            pltpu.VMEM((1, query_cols), f32),
            pltpu.VMEM((1, query_cols), f32),
            pltpu.VMEM((query_cols // HEAD_DIM, length, HEAD_DIM), bf16),
            pltpu.VMEM((levels, micros, count, rows, feats), bf16),
            pltpu.VMEM((micros, count, rows, feats), bf16),
            pltpu.VMEM((micros, chunks, count, rows, span), bf16),
            pltpu.VMEM((length, LANES), f32),
            pltpu.VMEM((length, query_cols), f32),
            pltpu.VMEM((length, kv_two), f32),
            pltpu.VMEM((micros, count, length, kv_two), bf16),
            pltpu.VMEM((KV_HEADS, length, HEAD_DIM), bf16),
            pltpu.VMEM((KV_HEADS, length, HEAD_DIM), bf16),
            pltpu.VMEM((length, query_cols), bf16),
            pltpu.VMEM((micros, chunks, minor, major, rows, span), bf16),
            pltpu.VMEM((micros, chunks, minor, major, rows, span), bf16),
            pltpu.VMEM((micros, chunks, major - 1, rows, span), bf16),
            pltpu.VMEM((micros, chunks, major, rows, span), bf16),
            pltpu.VMEM((chunks, rows, span), f32),
            pltpu.VMEM((1, width), f32),
            pltpu.VMEM((count, 1, width), f32),
            dma((4,)),
            dma((levels, micros)),
            dma((levels, micros)),
            dma((micros, major, major - 1)),
            dma((micros, chunks, major, minor - 1)),
            dma((micros, chunks, major)),
            dma((micros, chunks, count)),
            dma((micros, count - 1)),
            dma((micros, count)),
            dma((micros, chunks, minor - 1, major)),
            dma((micros, chunks, minor, major)),
            dma((micros, chunks, major - 1)),
            dma((micros, chunks, major)),
            dma((count - 1,)),
            dma((count,)),
            pltpu.SemaphoreType.REGULAR,
        ],
        compiler_params=pltpu.CompilerParams(
            collective_id=0, has_side_effects=True, vmem_limit_bytes=VMEM_MIB * 1024 * 1024
        ),
        name="layers",
    )(picked, gain, wq, wk, wv, wo, cos2, sin2, alpha)


VMEM_MIB = 40


PACK = 8
GROUP = 16


def pick_kernel(starts, marks, table, picked, tiles, sem):
    total = picked.shape[0]

    def fetch(token):
        start = pl.multiple_of(starts[token] * PACK, PACK)
        return pltpu.make_async_copy(
            table.at[pl.ds(start, PACK), :],
            tiles.at[pl.ds(pl.multiple_of(token * PACK, PACK), PACK), :],
            sem,
        )

    @pl.loop(0, total, unroll=8)
    def _(token):
        fetch(token).start()

    pltpu.make_async_copy(tiles, tiles, sem).wait()

    @pl.loop(0, total // GROUP)
    def _(group):
        here = pl.ds(pl.multiple_of(group * GROUP, GROUP), GROUP)
        depth = GROUP * PACK
        columns = lax.broadcasted_iota(jnp.int32, (GROUP, depth), 1)
        chosen = jnp.where(columns == marks[here, :], 1.0, 0.0).astype(jnp.bfloat16)
        block = tiles[pl.ds(pl.multiple_of(group * depth, depth), depth), :]
        picked[here, :] = jnp.dot(chosen, block, preferred_element_type=jnp.float32).astype(
            jnp.bfloat16
        )


def pick_rows(local_ids, table):
    total = local_ids.shape[0]
    vocab_rows, feats = table.shape
    inside = (local_ids >= 0) & (local_ids < vocab_rows)
    clipped = jnp.clip(local_ids, 0, vocab_rows - 1)
    place = (jnp.arange(total, dtype=jnp.int32) % GROUP) * PACK + clipped % PACK
    marks = jnp.where(inside, place, -1).reshape(total, 1)
    return pl.pallas_call(
        pick_kernel,
        out_shape=jax.ShapeDtypeStruct((total, feats), jnp.bfloat16),
        in_specs=[
            pl.BlockSpec(memory_space=pltpu.SMEM),
            pl.BlockSpec(memory_space=pltpu.VMEM),
            pl.BlockSpec(memory_space=pltpu.HBM),
        ],
        out_specs=pl.BlockSpec(memory_space=pltpu.VMEM),
        scratch_shapes=[
            pltpu.VMEM((total * PACK, feats), jnp.bfloat16),
            pltpu.SemaphoreType.DMA,
        ],
        compiler_params=pltpu.CompilerParams(vmem_limit_bytes=36 * 1024 * 1024),
        name="pick",
    )(clipped // PACK, marks, table)


def shards(token_ids, alpha_num, embed_table, norm_gain, w_query, w_key, w_value, w_out):
    tp_count = lax.axis_size("tp")
    section_count = lax.axis_size("section")
    section_index = lax.axis_index("section")
    micros, length = token_ids.shape
    vocab_rows, feats = embed_table.shape
    local_ids = (token_ids - section_index * vocab_rows).reshape(-1)
    picked = pick_rows(local_ids, embed_table)
    picked = picked.reshape(micros, tp_count, length // tp_count, feats)
    w_query, w_key, w_value, w_out = w_query[0], w_key[0], w_value[0], w_out[0]
    cosine, sine = rope_tables(length, HEAD_DIM)
    cos2 = jnp.concatenate([cosine, cosine], axis=1)
    sin2 = jnp.concatenate([-sine, sine], axis=1)
    alpha_exp = (alpha_num[0].astype(jnp.float32) / 10.0).reshape(1, 1)
    stored, scale_in, scale_out = run_layers(
        section_count,
        tp_count,
        picked,
        norm_gain,
        w_query,
        w_key.T,
        w_value.T,
        w_out,
        cos2,
        sin2,
        alpha_exp,
    )

    def smoothed(weights):
        return (weights.astype(jnp.float32) * scale_in[0][:, None]).astype(jnp.bfloat16)

    return (
        stored[None],
        scale_in,
        scale_out,
        smoothed(w_query)[None],
        smoothed(w_key)[None],
        smoothed(w_value)[None],
    )


def solution(mesh):
    return jax.shard_map(
        shards,
        mesh=mesh,
        in_specs=(
            P(),
            P(),
            P("section", "tp"),
            P("section", None),
            P("section", None, "tp"),
            P("section", None, "tp"),
            P("section", None, "tp"),
            P("section", "tp", None),
        ),
        out_specs=(
            P("section", None, "tp", None),
            P("section", None),
            P("section", "tp"),
            P("section", None, "tp"),
            P("section", None, "tp"),
            P("section", None, "tp"),
        ),
        check_vma=False,
    )
```
